32 devices in a mesh: blk: 32 (over z, y, x, core).
Axes of the slice: x: 2, y: 2, z: 4, core: 2. Of those that a mesh axis runs over, the one named last changes fastest.
Arguments:
- image_features: bfloat16 [8192, 1536], P('blk'), may hold values from -0.119628906 to 0.119628906
- head_weight: bfloat16 [1536, 1152], P('blk'), may hold values from -0.15625 to 0.15625
- text_embeds: bfloat16 [8192, 1152], P('blk'), may hold values from -0.29882812 to 0.29882812
- natural_exponent_factor: float32 [1], replicated, may hold values from 1.6 to 2.6
- logit_bias: float32 [1], replicated, may hold values from -4 to -1
Outputs:
- grad_features: bfloat16 [8192, 1536], P('blk')
- grad_text: bfloat16 [8192, 1152], P('blk')
- grad_weight: float32 [1536, 1152], P('blk')
The draws below stay inside these ranges and needn't reach their ends.
All inputs are finite; a program needn't handle non-finite values.
Results may differ from the reference program's by a relative error of at most 0.0085.
Values may be sent and summed in bfloat16 or wider, within the bound.
A program may use at most 64 MiB of HBM per device.

```python
import jax
import jax.numpy as jnp
from jax import lax

D = 1536
E = 1152
R = 256
S = 4
TOTAL = 8192
N_BLK = 32


def strengthened(entries, rng, source, target, blocks, factor):
    owner, partner = [(jnp.arange(entries.shape[axis_at]) // (entries.shape[axis_at] // blocks)).reshape([-1 if axis == axis_at else 1 for axis in range(entries.ndim)]) for axis_at in (source, target)]
    chosen = jax.random.permutation(rng, blocks)[partner]
    strong = (owner == chosen) | (owner == (partner + blocks // 2) % blocks)
    return jnp.where(strong, factor * entries, entries)


def levels(rng, extent, split, least, largest):
    def one(position, parts):
        steps = jax.random.uniform(jax.random.fold_in(jax.random.fold_in(rng, 6), position), (parts,), jnp.float32, least / len(split), largest / len(split))
        return jnp.repeat(jnp.exp(steps), extent[position] // parts).reshape((-1,) + (1,) * (len(extent) - position - 1))

    level = one(*split[0])
    for cut in split[1:]:
        level = level * one(*cut)
    return level


def bell_draw(stream_key, dims, scale, bound, pieces=(), kind=jnp.bfloat16):
    drawn = jax.random.normal(stream_key, dims, jnp.float32) * scale
    if len(pieces) > 0:
        drawn = levels(stream_key, dims, pieces, -0.22, 0.18) * drawn
    return jnp.clip(drawn, min=-bound, max=bound).astype(kind)


def heavy_noise(key, shape, spread, reach, pieces, heavy, kind=jnp.bfloat16):
    drawn = spread * jax.random.normal(key, shape, jnp.float32)
    if pieces:
        drawn = drawn * levels(key, shape, pieces, -0.22, 0.18)
    return jnp.clip(strengthened(drawn, jax.random.fold_in(key, 3), *heavy), -reach, reach).astype(kind)


def setup_inputs(seed: int = 0) -> dict:
    streams_of = jax.random.split(jax.random.key(seed), 6)
    return {
        "image_features": heavy_noise(streams_of[0], (TOTAL, D), 0.02, 0.119628906, ((0, 32),), (0, 1, 32, 2.75)),
        "head_weight": bell_draw(streams_of[1], (D, E), D ** -0.5, 0.15625, ((0, 32),)),
        "text_embeds": bell_draw(streams_of[2], (TOTAL, E), 0.05, 0.29882812, ((0, 32),)),
        "natural_exponent_factor": jnp.clip(jax.random.uniform(streams_of[3], (1,), jnp.float32, 1.6, 2.6), 1.6, 2.6),
        "logit_bias": jnp.clip(jax.random.uniform(streams_of[4], (1,), jnp.float32, -4.0, -1.0), -4.0, -1.0),
    }


epsilon = 1e-06

def normalize(rows):
    squares = lax.optimization_barrier(jnp.sum(rows * rows, axis=1, keepdims=True))
    length = jnp.sqrt(squares + epsilon)
    return (rows / length, length)

def similarity_derivative(picture_sample_group, caption_sample_group, similarity_multiplier, neighbour_distance, outer_dimension_size):
    similarity_matrix = similarity_multiplier * lax.dot_general(picture_sample_group, caption_sample_group, (((1,), (1,)), ((), ())), preferred_element_type=jnp.float32) + neighbour_distance
    if outer_dimension_size:
        matched = lax.broadcasted_iota(jnp.int32, similarity_matrix.shape, 0) == lax.broadcasted_iota(jnp.int32, similarity_matrix.shape, 1)
        match_polarity = jnp.where(matched, 1.0, -1.0).astype(jnp.float32)
    else:
        match_polarity = -jnp.ones(similarity_matrix.shape, jnp.float32)
    return (-similarity_multiplier * match_polarity * jax.nn.sigmoid(-match_polarity * similarity_matrix)).astype(jnp.bfloat16)

def project_back(grad, unit_rows, length):
    return (grad - unit_rows * lax.optimization_barrier(jnp.sum(unit_rows * grad, axis=1, keepdims=True))) / length

def reference(image_features, head_weight, text_embeds, natural_exponent_factor, logit_bias):
    embedded = jnp.dot(image_features, head_weight, preferred_element_type=jnp.float32)
    image_unit, image_length = normalize(embedded)
    picture_embedding_mapped = image_unit.astype(jnp.bfloat16)
    text_unit, text_length = normalize(text_embeds.astype(jnp.float32))
    text_low = text_unit.astype(jnp.bfloat16)
    similarity_multiplier = jnp.exp(natural_exponent_factor[0])
    neighbour_distance = logit_bias[0]
    image_blocks = picture_embedding_mapped.reshape(N_BLK, R, E)
    text_blocks = text_low.reshape(N_BLK, R, E)

    def pick_block(blocks, block_id):
        where_at = ((block_id + N_BLK) % N_BLK).astype(jnp.int32)
        return lax.dynamic_index_in_dim(blocks, where_at, 0, keepdims=False)

    def image_side(block_id):
        picture_sample_group = pick_block(image_blocks, block_id)
        summed = jnp.zeros((R, E), jnp.float32)
        for partition_portion in range(S):
            caption_sample_group = pick_block(text_blocks, block_id + partition_portion)
            mapping_matrix = similarity_derivative(picture_sample_group, caption_sample_group, similarity_multiplier, neighbour_distance, partition_portion == 0)
            summed = summed + jnp.dot(mapping_matrix, caption_sample_group, preferred_element_type=jnp.float32)
        return summed

    def text_side(block_id):
        caption_sample_group = pick_block(text_blocks, block_id)
        summed = jnp.zeros((R, E), jnp.float32)
        for partition_portion in range(S):
            picture_sample_group = pick_block(image_blocks, block_id - partition_portion)
            mapping_matrix = similarity_derivative(picture_sample_group, caption_sample_group, similarity_multiplier, neighbour_distance, partition_portion == 0)
            summed = summed + lax.dot_general(mapping_matrix, picture_sample_group, (((0,), (0,)), ((), ())), preferred_element_type=jnp.float32)
        return summed
    block_ids = jnp.arange(N_BLK, dtype=jnp.int32)
    image_grad = lax.map(image_side, block_ids).reshape(-1, E)
    text_grad = lax.map(text_side, block_ids).reshape(-1, E)
    embed_grad = project_back(image_grad, image_unit, image_length).astype(jnp.bfloat16)
    grad_text = project_back(text_grad, text_unit, text_length).astype(jnp.bfloat16)
    grad_features = lax.dot_general(embed_grad, head_weight, (((1,), (1,)), ((), ())), preferred_element_type=jnp.float32).astype(jnp.bfloat16)
    grad_weight = lax.dot_general(image_features, embed_grad, (((0,), (0,)), ((), ())), preferred_element_type=jnp.float32)
    return (grad_features, grad_text, grad_weight)
```

```python
import functools

import jax
import jax.numpy as jnp
from jax import lax
from jax.experimental import pallas as pl
from jax.experimental.pallas import tpu as pltpu
from jax.sharding import PartitionSpec as P

S = 4
epsilon = 1e-06
MESH = pl.DeviceIdType.MESH
F32 = jnp.float32
BF = jnp.bfloat16


def dot_nt(a, b):
    return lax.dot_general(a, b, (((1,), (1,)), ((), ())), preferred_element_type=F32)


def pair_grad(rows, cols, t, bias, own):
    logits = t * dot_nt(rows, cols) + bias
    if own:
        matched = lax.broadcasted_iota(jnp.int32, logits.shape, 0) == lax.broadcasted_iota(
            jnp.int32, logits.shape, 1
        )
        z = jnp.where(matched, 1.0, -1.0).astype(F32)
        return (-t * z * jax.nn.sigmoid(-z * logits)).astype(BF)
    return (t * jax.nn.sigmoid(logits)).astype(BF)


def sem_keys(depth):
    keys = [("z", d) for d in range(1, depth)]
    for d in range(depth):
        keys += [("x1", d), ("y1", d), ("y3", d, 0), ("y3", d, 1), ("x3", d, 0), ("x3", d, 1)]
        keys += [("w", d, i) for i in range(7)]
        keys += [(k, d) for k in ("g0", "g1a", "g1b", "g2a", "g2b", "g3")]
    for k in ("t", "i"):
        keys += [(k, "in", 0), (k, "in", 1), (k, "on", 0), (k, "on", 1), (k, "far")]
    return {k: i for i, k in enumerate(keys)}


def kernel(
    n, axis, keys,
    x_ref, w_ref, t_ref, lf_ref, bias_ref,
    gx_ref, gt_ref, gw_ref,
    w_all, text_low, text_in, image_low, image_in, xt, gz, from_core, to_core,
    s1a, s1b, r1a, r1b, s2a, s2b, r2a, r2b, s3, r3,
    send_sem, recv_sem,
):
    depth = n // 8
    rows, width = x_ref.shape
    own_rows, cols = w_ref.shape
    half = rows // 2
    ha = (cols // 128 + 1) // 2 * 128
    A, B = pl.ds(0, ha), pl.ds(ha, cols - ha)
    me = lax.axis_index(axis)
    core = lax.rem(me, 2)
    chip = me // 2
    x = lax.rem(chip, 2)
    y = lax.rem(chip // 2, 2)
    z = chip // 4

    def dev(z_, y_, x_, c_):
        return ((z_ * 2 + y_) * 2 + x_) * 2 + c_

    def up(d):
        return lax.rem(z + d, depth)

    def down(d):
        return lax.rem(z + depth - d, depth)

    xn, yn, partner = dev(z, y, 1 - x, core), dev(z, 1 - y, x, core), dev(z, y, x, 1 - core)
    sent = []

    def copy(src, dst, key, target):
        i = keys[key]
        return pltpu.make_async_remote_copy(
            src_ref=src, dst_ref=dst, send_sem=send_sem.at[i], recv_sem=recv_sem.at[i],
            device_id=(target,), device_id_type=MESH,
        )

    def send(src, dst, key, target):
        c = copy(src, dst, key, target)
        c.start()
        sent.append(c)

    def arrived(dst, key):
        copy(dst, dst, key, partner).wait_recv()

    barrier = pltpu.get_barrier_semaphore()
    for d in range(1, n):
        pl.semaphore_signal(barrier, inc=1, device_id=(lax.rem(me + d, n),), device_id_type=MESH)

    t = jnp.exp(jnp.full((1, 1), lf_ref[0], F32))
    bias = bias_ref[0]
    text = t_ref[...].astype(F32)
    text_length = jnp.sqrt(jnp.sum(text * text, axis=1, keepdims=True) + epsilon)
    text_low[...] = (text / text_length).astype(BF)
    w_all[me] = w_ref[...]

    pl.semaphore_wait(barrier, n - 1)

    send(w_ref.at[:, A], w_all.at[me, :, A], ("x1", 0), xn)
    send(w_ref.at[:, B], w_all.at[me, :, B], ("y1", 0), yn)
    for d in range(1, depth):
        send(w_ref, w_all.at[me], ("z", d), dev(up(d), y, x, core))
    send(w_ref.at[:, A], w_all.at[me, :, A], ("y3", 0, 0), yn)
    send(w_ref.at[:, B], w_all.at[me, :, B], ("x3", 0, 0), xn)
    send(w_ref, w_all.at[me], ("w", 0, 0), partner)

    below, above = lax.rem(me + n - 2, n), lax.rem(me + 2, n)

    def send_block(buf, slots, key, toward, far):
        base = toward - core
        for c in range(2):
            part = pl.ds(c * half, half)
            i = keys[(key, "in", 0)] + core
            cp = pltpu.make_async_remote_copy(
                src_ref=buf.at[part], dst_ref=slots.at[core, part],
                send_sem=send_sem.at[keys[(key, "in", c)]], recv_sem=recv_sem.at[i],
                device_id=(base + c,), device_id_type=MESH,
            )
            cp.start()
            sent.append(cp)
        send(buf, slots.at[2], (key, "far"), far)

    def swap_block(slots, key):
        part = pl.ds(pl.multiple_of(core * half, half), half)
        for q in range(2):
            arrived(slots.at[q, part], (key, "in", q))
            send(slots.at[q, part], slots.at[q, part], (key, "on", q), partner)

    def wait_block(slots, key, q):
        part = pl.ds(pl.multiple_of((1 - core) * half, half), half)
        arrived(slots.at[q, part], (key, "on", q))

    send_block(text_low, text_in, "t", below, lax.rem(me + n - 3 + 2 * core, n))

    xt[...] = x_ref[...].T

    def step_z(d):
        s = dev(down(d), y, x, core)
        arrived(w_all.at[s], ("z", d))
        send(w_all.at[s, :, A], w_all.at[s, :, A], ("x1", d), xn)
        send(w_all.at[s, :, B], w_all.at[s, :, B], ("y1", d), yn)
        send(w_all.at[s, :, A], w_all.at[s, :, A], ("y3", d, 0), yn)
        send(w_all.at[s, :, B], w_all.at[s, :, B], ("x3", d, 0), xn)
        send(w_all.at[s], w_all.at[s], ("w", d, 0), partner)

    def step_one(d):
        s = w_all.at[dev(down(d), y, 1 - x, core), :, A]
        arrived(s, ("x1", d))
        send(s, s, ("y3", d, 1), yn)
        send(s, s, ("w", d, 1), partner)
        s = w_all.at[dev(down(d), 1 - y, x, core), :, B]
        arrived(s, ("y1", d))
        send(s, s, ("x3", d, 1), xn)
        send(s, s, ("w", d, 2), partner)

    def step_two(d):
        for i, x_ in enumerate((x, 1 - x)):
            s = w_all.at[dev(down(d), 1 - y, x_, core), :, A]
            arrived(s, ("y3", d, i))
            send(s, s, ("w", d, 3 + i), partner)
        for i, y_ in enumerate((y, 1 - y)):
            s = w_all.at[dev(down(d), y_, 1 - x, core), :, B]
            arrived(s, ("x3", d, i))
            send(s, s, ("w", d, 5 + i), partner)

    for step in range(depth + 2):
        if 1 <= step < depth:
            step_z(step)
        if 0 <= step - 1 < depth:
            step_one(step - 1)
        if 0 <= step - 2 < depth:
            step_two(step - 2)

    other = 1 - core
    for d in range(depth):
        zs = down(d)
        arrived(w_all.at[dev(zs, y, x, other)], ("w", d, 0))
        arrived(w_all.at[dev(zs, y, 1 - x, other), :, A], ("w", d, 1))
        arrived(w_all.at[dev(zs, 1 - y, x, other), :, B], ("w", d, 2))
        for i, x_ in enumerate((x, 1 - x)):
            arrived(w_all.at[dev(zs, 1 - y, x_, other), :, A], ("w", d, 3 + i))
        for i, y_ in enumerate((y, 1 - y)):
            arrived(w_all.at[dev(zs, y_, 1 - x, other), :, B], ("w", d, 5 + i))

    weight = w_all[...].reshape(n * own_rows, cols)
    embedded = jnp.dot(x_ref[...], weight, preferred_element_type=F32)
    image_length = jnp.sqrt(jnp.sum(embedded * embedded, axis=1, keepdims=True) + epsilon)
    image_unit = embedded / image_length
    image_low[...] = image_unit.astype(BF)
    mine = image_low[...]
    own_text = text_low[...]

    grad = pair_grad(mine, own_text, t, bias, True)
    image_grad = jnp.dot(grad, own_text, preferred_element_type=F32)
    send_block(image_low, image_in, "i", above, lax.rem(me + 1 + 2 * core, n))

    swap_block(text_in, "t")
    arrived(text_in.at[2], ("t", "far"))
    for q in (2, 0, 1):
        if q < 2:
            wait_block(text_in, "t", q)
        block = text_in[q]
        image_grad += jnp.dot(
            pair_grad(mine, block, t, bias, False), block, preferred_element_type=F32
        )
    along = jnp.sum(image_unit * image_grad, axis=1, keepdims=True)
    embed_grad = ((image_grad - image_unit * along) / image_length).astype(BF)

    order = [d for d in range(1, depth)] + [0]
    group = 8 * own_rows
    for d in order:
        lhs = xt[pl.ds(pl.multiple_of(up(d) * group, group), group), :]
        part = jnp.dot(lhs, embed_grad, preferred_element_type=F32)
        gz[d] = part.reshape(4, 2, own_rows, cols)
        for c in range(4):
            to_core[d, c] = gz[d, c, other].astype(BF)
        send(to_core.at[d], from_core.at[d], ("g0", d), partner)

    def base(d, c, cut):
        return gz[d, c, core, :, cut] + from_core[d, c, :, cut].astype(F32)

    swap_block(image_in, "i")
    gx_ref[...] = dot_nt(embed_grad, weight).astype(BF)

    for d in order:
        arrived(from_core.at[d], ("g0", d))
        for i in range(2):
            s1a[d, i] = base(d, (1 - y) * 2 + i, A).astype(BF)
            s1b[d, i] = base(d, i * 2 + 1 - x, B).astype(BF)
        send(s1a.at[d], r1a.at[d], ("g1a", d), yn)
        send(s1b.at[d], r1b.at[d], ("g1b", d), xn)

    text_grad = jnp.dot(
        pair_grad(own_text, mine, t, bias, True), mine, preferred_element_type=F32
    )

    def stage_two(d):
        arrived(r1a.at[d], ("g1a", d))
        s2a[d] = (base(d, y * 2 + 1 - x, A) + r1a[d, 1 - x].astype(F32)).astype(BF)
        send(s2a.at[d], r2a.at[d], ("g2a", d), xn)
        arrived(r1b.at[d], ("g1b", d))
        s2b[d] = (base(d, (1 - y) * 2 + x, B) + r1b[d, 1 - y].astype(F32)).astype(BF)
        send(s2b.at[d], r2b.at[d], ("g2b", d), yn)

    def stage_three(d):
        here = y * 2 + x
        arrived(r2a.at[d], ("g2a", d))
        arrived(r2b.at[d], ("g2b", d))
        left = base(d, here, A) + r1a[d, x].astype(F32) + r2a[d].astype(F32)
        right = base(d, here, B) + r1b[d, y].astype(F32) + r2b[d].astype(F32)
        if d == 0:
            gw_ref[:, A] = left
            gw_ref[:, B] = right
        else:
            s3[d, :, A] = left.astype(BF)
            s3[d, :, B] = right.astype(BF)
            send(s3.at[d], r3.at[d], ("g3", d), dev(up(d), y, x, core))

    for i, d in enumerate(order):
        stage_two(d)
        if i >= 1:
            stage_three(order[i - 1])

    for q in (2, 0, 1):
        if q < 2:
            wait_block(image_in, "i", q)
        else:
            arrived(image_in.at[2], ("i", "far"))
        block = image_in[q]
        text_grad += jnp.dot(
            pair_grad(own_text, block, t, bias, False), block, preferred_element_type=F32
        )
    text_unit = t_ref[...].astype(F32) / text_length
    along = jnp.sum(text_unit * text_grad, axis=1, keepdims=True)
    gt_ref[...] = ((text_grad - text_unit * along) / text_length).astype(BF)

    stage_three(order[-1])
    total = gw_ref[...]
    for d in range(1, depth):
        arrived(r3.at[d], ("g3", d))
        total += r3[d].astype(F32)
    gw_ref[...] = total
    for c in sent:
        c.wait_send()


def fused(n, axis, image_features, head_weight, text_embeds, factor, bias):
    depth = n // 8
    rows, width = image_features.shape
    own_rows, cols = head_weight.shape
    keys = sem_keys(depth)
    ha = (cols // 128 + 1) // 2 * 128
    hb = cols - ha
    vmem = pl.BlockSpec(memory_space=pltpu.VMEM)
    smem = pl.BlockSpec(memory_space=pltpu.SMEM)
    scratch = [
        ((n, own_rows, cols), BF),
        ((rows, cols), BF),
        ((3, rows, cols), BF),
        ((rows, cols), BF),
        ((3, rows, cols), BF),
        ((width, rows), BF),
        ((depth, 4, 2, own_rows, cols), F32),
        ((depth, 4, own_rows, cols), BF),
        ((depth, 4, own_rows, cols), BF),
        ((depth, 2, own_rows, ha), BF),
        ((depth, 2, own_rows, hb), BF),
        ((depth, 2, own_rows, ha), BF),
        ((depth, 2, own_rows, hb), BF),
        ((depth, own_rows, ha), BF),
        ((depth, own_rows, hb), BF),
        ((depth, own_rows, ha), BF),
        ((depth, own_rows, hb), BF),
        ((depth, own_rows, cols), BF),
        ((depth, own_rows, cols), BF),
    ]
    return pl.pallas_call(
        functools.partial(kernel, n, axis, keys),
        out_shape=(
            jax.ShapeDtypeStruct((rows, width), BF),
            jax.ShapeDtypeStruct((rows, cols), BF),
            jax.ShapeDtypeStruct((own_rows, cols), F32),
        ),
        in_specs=[vmem, vmem, vmem, smem, smem],
        out_specs=(vmem, vmem, vmem),
        scratch_shapes=[pltpu.VMEM(s, d) for s, d in scratch]
        + [pltpu.SemaphoreType.DMA((len(keys),))] * 2,
        compiler_params=pltpu.CompilerParams(
            collective_id=0, has_side_effects=True, vmem_limit_bytes=60 * 2**20
        ),
    )(image_features, head_weight, text_embeds, factor, bias)


def passed_along(block, axis, distance):
    devices = range(lax.axis_size(axis))
    route = [((i - distance) % len(devices), i) for i in devices]
    return lax.ppermute(block, axis, route)


def normalize(rows):
    squares = jnp.sum(rows * rows, axis=1, keepdims=True)
    length = jnp.sqrt(squares + epsilon)
    return (rows / length, length)


def similarity_derivative(
    picture_sample_group,
    caption_sample_group,
    similarity_multiplier,
    neighbour_distance,
    outer_dimension_size,
):
    similarity_matrix = (
        similarity_multiplier
        * lax.dot_general(
            picture_sample_group,
            caption_sample_group,
            (((1,), (1,)), ((), ())),
            preferred_element_type=jnp.float32,
        )
        + neighbour_distance
    )
    if outer_dimension_size:
        matched = lax.broadcasted_iota(
            jnp.int32, similarity_matrix.shape, 0
        ) == lax.broadcasted_iota(jnp.int32, similarity_matrix.shape, 1)
        match_polarity = jnp.where(matched, 1.0, -1.0).astype(jnp.float32)
    else:
        match_polarity = -jnp.ones(similarity_matrix.shape, jnp.float32)
    return (
        -similarity_multiplier
        * match_polarity
        * jax.nn.sigmoid(-match_polarity * similarity_matrix)
    ).astype(jnp.bfloat16)


def project_back(grad, unit_rows, length):
    return (grad - unit_rows * jnp.sum(unit_rows * grad, axis=1, keepdims=True)) / length


def by_collectives(image_features, head_weight, text_embeds, natural_exponent_factor, logit_bias):
    full_weight = lax.all_gather(head_weight, "blk", axis=0, tiled=True)
    embedded = jnp.dot(image_features, full_weight, preferred_element_type=jnp.float32)
    image_unit, image_length = normalize(embedded)
    picture_embedding_mapped = image_unit.astype(jnp.bfloat16)
    text_unit, text_length = normalize(text_embeds.astype(jnp.float32))
    text_low = text_unit.astype(jnp.bfloat16)
    similarity_multiplier = jnp.exp(natural_exponent_factor[0])
    neighbour_distance = logit_bias[0]
    image_grad = jnp.zeros(image_unit.shape, jnp.float32)
    current_neighbour_tile = text_low
    for partition_portion in range(S):
        mapping_matrix = similarity_derivative(
            picture_embedding_mapped,
            current_neighbour_tile,
            similarity_multiplier,
            neighbour_distance,
            partition_portion == 0,
        )
        image_grad = image_grad + jnp.dot(
            mapping_matrix, current_neighbour_tile, preferred_element_type=jnp.float32
        )
        if partition_portion + 1 < S:
            current_neighbour_tile = passed_along(current_neighbour_tile, "blk", -1)
    text_grad = jnp.zeros(text_unit.shape, jnp.float32)
    passing = picture_embedding_mapped
    for partition_portion in range(S):
        mapping_matrix = similarity_derivative(
            passing, text_low, similarity_multiplier, neighbour_distance, partition_portion == 0
        )
        text_grad = text_grad + lax.dot_general(
            mapping_matrix, passing, (((0,), (0,)), ((), ())), preferred_element_type=jnp.float32
        )
        if partition_portion + 1 < S:
            passing = passed_along(passing, "blk", 1)
    embed_grad = project_back(image_grad, image_unit, image_length).astype(jnp.bfloat16)
    grad_text = project_back(text_grad, text_unit, text_length).astype(jnp.bfloat16)
    grad_features = lax.dot_general(
        embed_grad, full_weight, (((1,), (1,)), ((), ())), preferred_element_type=jnp.float32
    ).astype(jnp.bfloat16)
    grad_weight = lax.psum_scatter(
        lax.dot_general(
            image_features, embed_grad, (((0,), (0,)), ((), ())), preferred_element_type=jnp.float32
        ),
        "blk",
        scatter_dimension=0,
        tiled=True,
    )
    return (grad_features, grad_text, grad_weight)


def on_device(image_features, head_weight, text_embeds, natural_exponent_factor, logit_bias):
    n = lax.axis_size("blk")
    whole_tiles = head_weight.shape[0] % 16 == 0 and n % 8 == 0 and n > 8
    run = functools.partial(fused, n, "blk") if whole_tiles else by_collectives
    return run(image_features, head_weight, text_embeds, natural_exponent_factor, logit_bias)


def solution(mesh):
    return jax.shard_map(
        on_device,
        mesh=mesh,
        in_specs=(P("blk", None), P("blk", None), P("blk", None), P(), P()),
        out_specs=(P("blk", None), P("blk", None), P("blk", None)),
        check_vma=False,
    )
```

```python
import functools

import jax
import jax.numpy as jnp
from jax import lax
from jax.experimental import pallas as pl
from jax.experimental.pallas import tpu as pltpu
from jax.sharding import PartitionSpec as P

S = 4
epsilon = 1e-06
MESH = pl.DeviceIdType.MESH
F32 = jnp.float32
BF = jnp.bfloat16


def dot_nt(a, b):
    return lax.dot_general(a, b, (((1,), (1,)), ((), ())), preferred_element_type=F32)


def pair_grad(rows, cols, t, bias, own):
    logits = t * dot_nt(rows, cols) + bias
    if own:
        matched = lax.broadcasted_iota(jnp.int32, logits.shape, 0) == lax.broadcasted_iota(
            jnp.int32, logits.shape, 1
        )
        z = jnp.where(matched, 1.0, -1.0).astype(F32)
        return (-t * z * jax.nn.sigmoid(-z * logits)).astype(BF)
    return (t * jax.nn.sigmoid(logits)).astype(BF)


def sem_keys(depth):
    keys = ["za", "zb", "g3a", "g3b"] + [("z", d) for d in range(1, depth)]
    for d in range(depth):
        keys += [("x1", d), ("y1", d), ("y3", d, 0), ("y3", d, 1), ("x3", d, 0), ("x3", d, 1)]
        keys += [("w", d, i) for i in range(8)]
        keys += [(k, d) for k in ("g0", "g1a", "g1b", "g2a", "g2b")]
    for k in ("t", "i"):
        keys += [(k, "in", 0), (k, "in", 1), (k, "on", 0), (k, "on", 1), (k, "far")]
    return {k: i for i, k in enumerate(keys)}


def kernel(
    n, axis, keys,
    x_ref, w_ref, t_ref, lf_ref, bias_ref,
    gx_ref, gt_ref, gw_ref,
    w_all, text_low, text_in, image_low, image_in, xt, gz, from_core, to_core,
    s1a, s1b, r1a, r1b, s2a, s2b, r2a, r2b, s3a, s3b, r3a, r3b,
    send_sem, recv_sem,
):
    depth = n // 8
    opp = depth // 2
    near = [d for d in range(1, depth) if d != opp]
    rows, width = x_ref.shape
    own_rows, cols = w_ref.shape
    half = rows // 2
    ha = (cols // 128 + 1) // 2 * 128
    A, B = pl.ds(0, ha), pl.ds(ha, cols - ha)
    me = lax.axis_index(axis)
    core = lax.rem(me, 2)
    chip = me // 2
    x = lax.rem(chip, 2)
    y = lax.rem(chip // 2, 2)
    z = chip // 4

    def dev(z_, y_, x_, c_):
        return ((z_ * 2 + y_) * 2 + x_) * 2 + c_

    def up(d):
        return lax.rem(z + d, depth)

    def down(d):
        return lax.rem(z + depth - d, depth)

    xn, yn, partner = dev(z, y, 1 - x, core), dev(z, 1 - y, x, core), dev(z, y, x, 1 - core)
    sent = []

    def copy(src, dst, key, target):
        i = keys[key]
        return pltpu.make_async_remote_copy(
            src_ref=src, dst_ref=dst, send_sem=send_sem.at[i], recv_sem=recv_sem.at[i],
            device_id=(target,), device_id_type=MESH,
        )

    def send(src, dst, key, target):
        c = copy(src, dst, key, target)
        c.start()
        sent.append(c)

    def arrived(dst, key):
        copy(dst, dst, key, partner).wait_recv()

    barrier = pltpu.get_barrier_semaphore()
    for d in range(1, n):
        pl.semaphore_signal(barrier, inc=1, device_id=(lax.rem(me + d, n),), device_id_type=MESH)

    t = jnp.exp(jnp.full((1, 1), lf_ref[0], F32))
    bias = bias_ref[0]
    text = t_ref[...].astype(F32)
    text_length = jnp.sqrt(jnp.sum(text * text, axis=1, keepdims=True) + epsilon)
    text_low[...] = (text / text_length).astype(BF)
    w_all[me] = w_ref[...]

    pl.semaphore_wait(barrier, n - 1)

    send(w_ref.at[:, A], w_all.at[me, :, A], ("x1", 0), xn)
    send(w_ref.at[:, B], w_all.at[me, :, B], ("y1", 0), yn)
    for d in near:
        send(w_ref, w_all.at[me], ("z", d), dev(up(d), y, x, core))
    send(w_ref.at[:, A], w_all.at[me, :, A], ("y3", 0, 0), yn)
    send(w_ref.at[:, B], w_all.at[me, :, B], ("x3", 0, 0), xn)
    send(w_ref, w_all.at[me], ("w", 0, 0), partner)

    below, above = lax.rem(me + n - 2, n), lax.rem(me + 2, n)

    def send_block(buf, slots, key, toward, far):
        base = toward - core
        for c in range(2):
            part = pl.ds(c * half, half)
            i = keys[(key, "in", 0)] + core
            cp = pltpu.make_async_remote_copy(
                src_ref=buf.at[part], dst_ref=slots.at[core, part],
                send_sem=send_sem.at[keys[(key, "in", c)]], recv_sem=recv_sem.at[i],
                device_id=(base + c,), device_id_type=MESH,
            )
            cp.start()
            sent.append(cp)
        send(buf, slots.at[2], (key, "far"), far)

    def swap_block(slots, key):
        part = pl.ds(pl.multiple_of(core * half, half), half)
        for q in range(2):
            arrived(slots.at[q, part], (key, "in", q))
            send(slots.at[q, part], slots.at[q, part], (key, "on", q), partner)

    def wait_block(slots, key, q):
        part = pl.ds(pl.multiple_of((1 - core) * half, half), half)
        arrived(slots.at[q, part], (key, "on", q))


    xt[...] = x_ref[...].T

    def onward(part, d, key_a, key_b):
        if key_a is not None and d == opp - 1:
            send(part(A), part(A), key_a, dev(up(1), y, x, core))
        if key_b is not None and d == opp + 1:
            send(part(B), part(B), key_b, dev(down(1), y, x, core))

    def step_z(d):
        s = dev(down(d), y, x, core)

        def part(cut):
            return w_all.at[s, :, cut]

        if d == opp:
            arrived(part(A), "za")
            send(part(A), part(A), ("y3", d, 0), yn)
            send(part(A), part(A), ("w", d, 0), partner)
            arrived(part(B), "zb")
            send(part(B), part(B), ("x3", d, 0), xn)
            send(part(B), part(B), ("w", d, 7), partner)
            return
        arrived(w_all.at[s], ("z", d))
        onward(part, d, "za", "zb")
        send(part(A), part(A), ("y3", d, 0), yn)
        send(part(B), part(B), ("x3", d, 0), xn)
        send(w_all.at[s], w_all.at[s], ("w", d, 0), partner)

    def step_one(d):
        def side(cut):
            return w_all.at[dev(down(d), y, 1 - x, core), :, cut]

        def front(cut):
            return w_all.at[dev(down(d), 1 - y, x, core), :, cut]

        s = side(A)
        arrived(s, ("x1", d))
        if d == 0:
            for e in near:
                send(s, s, ("x1", e), dev(up(e), y, x, core))
        onward(side, d, ("x1", opp), None)
        send(s, s, ("y3", d, 1), yn)
        send(s, s, ("w", d, 1), partner)
        s = front(B)
        arrived(s, ("y1", d))
        if d == 0:
            for e in near:
                send(s, s, ("y1", e), dev(up(e), y, x, core))
        onward(front, d, None, ("y1", opp))
        send(s, s, ("x3", d, 1), xn)
        send(s, s, ("w", d, 2), partner)

    def step_two(d):
        for i, x_ in enumerate((x, 1 - x)):
            s = w_all.at[dev(down(d), 1 - y, x_, core), :, A]
            arrived(s, ("y3", d, i))
            send(s, s, ("w", d, 3 + i), partner)
        for i, y_ in enumerate((y, 1 - y)):
            s = w_all.at[dev(down(d), y_, 1 - x, core), :, B]
            arrived(s, ("x3", d, i))
            send(s, s, ("w", d, 5 + i), partner)

    step_one(0)
    for d in near:
        step_z(d)
    for d in near:
        step_one(d)
    step_z(opp)
    step_one(opp)
    for d in [0] + near + [opp]:
        step_two(d)

    send_block(text_low, text_in, "t", below, lax.rem(me + n - 3 + 2 * core, n))
    other = 1 - core
    for d in range(depth):
        zs = down(d)
        if d == opp:
            arrived(w_all.at[dev(zs, y, x, other), :, A], ("w", d, 0))
            arrived(w_all.at[dev(zs, y, x, other), :, B], ("w", d, 7))
        else:
            arrived(w_all.at[dev(zs, y, x, other)], ("w", d, 0))
        arrived(w_all.at[dev(zs, y, 1 - x, other), :, A], ("w", d, 1))
        arrived(w_all.at[dev(zs, 1 - y, x, other), :, B], ("w", d, 2))
        for i, x_ in enumerate((x, 1 - x)):
            arrived(w_all.at[dev(zs, 1 - y, x_, other), :, A], ("w", d, 3 + i))
        for i, y_ in enumerate((y, 1 - y)):
            arrived(w_all.at[dev(zs, y_, 1 - x, other), :, B], ("w", d, 5 + i))

    weight = w_all[...].reshape(n * own_rows, cols)
    embedded = jnp.dot(x_ref[...], weight, preferred_element_type=F32)
    image_length = jnp.sqrt(jnp.sum(embedded * embedded, axis=1, keepdims=True) + epsilon)
    image_unit = embedded / image_length
    image_low[...] = image_unit.astype(BF)
    mine = image_low[...]
    own_text = text_low[...]

    grad = pair_grad(mine, own_text, t, bias, True)
    image_grad = jnp.dot(grad, own_text, preferred_element_type=F32)
    send_block(image_low, image_in, "i", above, lax.rem(me + 1 + 2 * core, n))

    swap_block(text_in, "t")
    arrived(text_in.at[2], ("t", "far"))
    for q in (2, 0, 1):
        if q < 2:
            wait_block(text_in, "t", q)
        block = text_in[q]
        image_grad += jnp.dot(
            pair_grad(mine, block, t, bias, False), block, preferred_element_type=F32
        )
    along = jnp.sum(image_unit * image_grad, axis=1, keepdims=True)
    embed_grad = ((image_grad - image_unit * along) / image_length).astype(BF)

    order = [opp] + near + [0]
    group = 8 * own_rows
    for d in order:
        lhs = xt[pl.ds(pl.multiple_of(up(d) * group, group), group), :]
        part = jnp.dot(lhs, embed_grad, preferred_element_type=F32)
        gz[d] = part.reshape(4, 2, own_rows, cols)
        for c in range(4):
            to_core[d, c] = gz[d, c, other].astype(BF)
        send(to_core.at[d], from_core.at[d], ("g0", d), partner)

    def base(d, c, cut):
        return gz[d, c, core, :, cut] + from_core[d, c, :, cut].astype(F32)

    swap_block(image_in, "i")
    gx_ref[...] = dot_nt(embed_grad, weight).astype(BF)

    for d in order:
        arrived(from_core.at[d], ("g0", d))
        for i in range(2):
            s1a[d, i] = base(d, (1 - y) * 2 + i, A).astype(BF)
            s1b[d, i] = base(d, i * 2 + 1 - x, B).astype(BF)
        send(s1a.at[d], r1a.at[d], ("g1a", d), yn)
        send(s1b.at[d], r1b.at[d], ("g1b", d), xn)

    text_grad = jnp.dot(
        pair_grad(own_text, mine, t, bias, True), mine, preferred_element_type=F32
    )

    def stage_two(d):
        arrived(r1a.at[d], ("g1a", d))
        arrived(r1b.at[d], ("g1b", d))
        if d == opp - 1:
            arrived(r2a.at[opp], ("g2a", opp))
        if d == opp + 1:
            arrived(r2b.at[opp], ("g2b", opp))
        for i in range(2):
            left = base(d, y * 2 + i, A) + r1a[d, i].astype(F32)
            right = base(d, i * 2 + x, B) + r1b[d, i].astype(F32)
            if d == opp - 1:
                left += r2a[opp, i].astype(F32)
            if d == opp + 1:
                right += r2b[opp, i].astype(F32)
            s2a[d, i] = left.astype(BF)
            s2b[d, i] = right.astype(BF)
        ta, tb = (up(1), down(1)) if d == opp else (up(d), up(d))
        send(s2a.at[d], r2a.at[d], ("g2a", d), dev(ta, y, x, core))
        send(s2b.at[d], r2b.at[d], ("g2b", d), dev(tb, y, x, core))

    def gathered(i, j):
        left = base(0, y * 2 + i, A) + r1a[0, i].astype(F32)
        right = base(0, j * 2 + x, B) + r1b[0, j].astype(F32)
        for d in near:
            left += r2a[d, i].astype(F32)
            right += r2b[d, j].astype(F32)
        return left, right

    for d in [opp] + near:
        stage_two(d)

    for q in (2, 0, 1):
        if q < 2:
            wait_block(image_in, "i", q)
        else:
            arrived(image_in.at[2], ("i", "far"))
        block = image_in[q]
        text_grad += jnp.dot(
            pair_grad(own_text, block, t, bias, False), block, preferred_element_type=F32
        )
    arrived(r1a.at[0], ("g1a", 0))
    arrived(r1b.at[0], ("g1b", 0))
    for d in near:
        arrived(r2a.at[d], ("g2a", d))
        arrived(r2b.at[d], ("g2b", d))
    left, right = gathered(1 - x, 1 - y)
    s3a[...] = left.astype(BF)
    s3b[...] = right.astype(BF)
    send(s3a, r3a, "g3a", xn)
    send(s3b, r3b, "g3b", yn)
    left, right = gathered(x, y)
    gw_ref[:, A] = left
    gw_ref[:, B] = right
    text_unit = t_ref[...].astype(F32) / text_length
    along = jnp.sum(text_unit * text_grad, axis=1, keepdims=True)
    gt_ref[...] = ((text_grad - text_unit * along) / text_length).astype(BF)

    arrived(r3a, "g3a")
    arrived(r3b, "g3b")
    gw_ref[:, A] += r3a[...].astype(F32)
    gw_ref[:, B] += r3b[...].astype(F32)
    for c in sent:
        c.wait_send()


def fused(n, axis, image_features, head_weight, text_embeds, factor, bias):
    depth = n // 8
    rows, width = image_features.shape
    own_rows, cols = head_weight.shape
    keys = sem_keys(depth)
    ha = (cols // 128 + 1) // 2 * 128
    hb = cols - ha
    vmem = pl.BlockSpec(memory_space=pltpu.VMEM)
    smem = pl.BlockSpec(memory_space=pltpu.SMEM)
    scratch = [
        ((n, own_rows, cols), BF),
        ((rows, cols), BF),
        ((3, rows, cols), BF),
        ((rows, cols), BF),
        ((3, rows, cols), BF),
        ((width, rows), BF),
        ((depth, 4, 2, own_rows, cols), F32),
        ((depth, 4, own_rows, cols), BF),
        ((depth, 4, own_rows, cols), BF),
        ((depth, 2, own_rows, ha), BF),
        ((depth, 2, own_rows, hb), BF),
        ((depth, 2, own_rows, ha), BF),
        ((depth, 2, own_rows, hb), BF),
        ((depth, 2, own_rows, ha), BF),
        ((depth, 2, own_rows, hb), BF),
        ((depth, 2, own_rows, ha), BF),
        ((depth, 2, own_rows, hb), BF),
        ((own_rows, ha), BF),
        ((own_rows, hb), BF),
        ((own_rows, ha), BF),
        ((own_rows, hb), BF),
    ]
    return pl.pallas_call(
        functools.partial(kernel, n, axis, keys),
        out_shape=(
            jax.ShapeDtypeStruct((rows, width), BF),
            jax.ShapeDtypeStruct((rows, cols), BF),
            jax.ShapeDtypeStruct((own_rows, cols), F32),
        ),
        in_specs=[vmem, vmem, vmem, smem, smem],
        out_specs=(vmem, vmem, vmem),
        scratch_shapes=[pltpu.VMEM(s, d) for s, d in scratch]
        + [pltpu.SemaphoreType.DMA((len(keys),))] * 2,
        compiler_params=pltpu.CompilerParams(
            collective_id=0, has_side_effects=True, vmem_limit_bytes=60 * 2**20
        ),
    )(image_features, head_weight, text_embeds, factor, bias)


def passed_along(block, axis, distance):
    devices = range(lax.axis_size(axis))
    route = [((i - distance) % len(devices), i) for i in devices]
    return lax.ppermute(block, axis, route)


def normalize(rows):
    squares = jnp.sum(rows * rows, axis=1, keepdims=True)
    length = jnp.sqrt(squares + epsilon)
    return (rows / length, length)


def similarity_derivative(
    picture_sample_group,
    caption_sample_group,
    similarity_multiplier,
    neighbour_distance,
    outer_dimension_size,
):
    similarity_matrix = (
        similarity_multiplier
        * lax.dot_general(
            picture_sample_group,
            caption_sample_group,
            (((1,), (1,)), ((), ())),
            preferred_element_type=jnp.float32,
        )
        + neighbour_distance
    )
    if outer_dimension_size:
        matched = lax.broadcasted_iota(
            jnp.int32, similarity_matrix.shape, 0
        ) == lax.broadcasted_iota(jnp.int32, similarity_matrix.shape, 1)
        match_polarity = jnp.where(matched, 1.0, -1.0).astype(jnp.float32)
    else:
        match_polarity = -jnp.ones(similarity_matrix.shape, jnp.float32)
    return (
        -similarity_multiplier
        * match_polarity
        * jax.nn.sigmoid(-match_polarity * similarity_matrix)
    ).astype(jnp.bfloat16)


def project_back(grad, unit_rows, length):
    return (grad - unit_rows * jnp.sum(unit_rows * grad, axis=1, keepdims=True)) / length


def by_collectives(image_features, head_weight, text_embeds, natural_exponent_factor, logit_bias):
    full_weight = lax.all_gather(head_weight, "blk", axis=0, tiled=True)
    embedded = jnp.dot(image_features, full_weight, preferred_element_type=jnp.float32)
    image_unit, image_length = normalize(embedded)
    picture_embedding_mapped = image_unit.astype(jnp.bfloat16)
    text_unit, text_length = normalize(text_embeds.astype(jnp.float32))
    text_low = text_unit.astype(jnp.bfloat16)
    similarity_multiplier = jnp.exp(natural_exponent_factor[0])
    neighbour_distance = logit_bias[0]
    image_grad = jnp.zeros(image_unit.shape, jnp.float32)
    current_neighbour_tile = text_low
    for partition_portion in range(S):
        mapping_matrix = similarity_derivative(
            picture_embedding_mapped,
            current_neighbour_tile,
            similarity_multiplier,
            neighbour_distance,
            partition_portion == 0,
        )
        image_grad = image_grad + jnp.dot(
            mapping_matrix, current_neighbour_tile, preferred_element_type=jnp.float32
        )
        if partition_portion + 1 < S:
            current_neighbour_tile = passed_along(current_neighbour_tile, "blk", -1)
    text_grad = jnp.zeros(text_unit.shape, jnp.float32)
    passing = picture_embedding_mapped
    for partition_portion in range(S):
        mapping_matrix = similarity_derivative(
            passing, text_low, similarity_multiplier, neighbour_distance, partition_portion == 0
        )
        text_grad = text_grad + lax.dot_general(
            mapping_matrix, passing, (((0,), (0,)), ((), ())), preferred_element_type=jnp.float32
        )
        if partition_portion + 1 < S:
            passing = passed_along(passing, "blk", 1)
    embed_grad = project_back(image_grad, image_unit, image_length).astype(jnp.bfloat16)
    grad_text = project_back(text_grad, text_unit, text_length).astype(jnp.bfloat16)
    grad_features = lax.dot_general(
        embed_grad, full_weight, (((1,), (1,)), ((), ())), preferred_element_type=jnp.float32
    ).astype(jnp.bfloat16)
    grad_weight = lax.psum_scatter(
        lax.dot_general(
            image_features, embed_grad, (((0,), (0,)), ((), ())), preferred_element_type=jnp.float32
        ),
        "blk",
        scatter_dimension=0,
        tiled=True,
    )
    return (grad_features, grad_text, grad_weight)


def on_device(image_features, head_weight, text_embeds, natural_exponent_factor, logit_bias):
    n = lax.axis_size("blk")
    whole_tiles = head_weight.shape[0] % 16 == 0 and n % 16 == 0 and n > 16
    run = functools.partial(fused, n, "blk") if whole_tiles else by_collectives
    return run(image_features, head_weight, text_embeds, natural_exponent_factor, logit_bias)


def solution(mesh):
    return jax.shard_map(
        on_device,
        mesh=mesh,
        in_specs=(P("blk", None), P("blk", None), P("blk", None), P(), P()),
        out_specs=(P("blk", None), P("blk", None), P("blk", None)),
        check_vma=False,
    )
```

```python
import functools

import jax
import jax.numpy as jnp
from jax import lax
from jax.experimental import pallas as pl
from jax.experimental.pallas import tpu as pltpu
from jax.sharding import PartitionSpec as P

S = 4
epsilon = 1e-06
MESH = pl.DeviceIdType.MESH
F32 = jnp.float32
BF = jnp.bfloat16


def dot_nt(a, b):
    return lax.dot_general(a, b, (((1,), (1,)), ((), ())), preferred_element_type=F32)


def pair_grad(rows, cols, t, bias, own):
    logits = t * dot_nt(rows, cols) + bias
    if own:
        matched = lax.broadcasted_iota(jnp.int32, logits.shape, 0) == lax.broadcasted_iota(
            jnp.int32, logits.shape, 1
        )
        z = jnp.where(matched, 1.0, -1.0).astype(F32)
        return (-t * z * jax.nn.sigmoid(-z * logits)).astype(BF)
    return (t * jax.nn.sigmoid(logits)).astype(BF)


def sem_keys(depth):
    keys = ["za", "zb", "g3a", "g3b"] + [("z", d) for d in range(1, depth)]
    for d in range(depth):
        keys += [("x1", d), ("y1", d), ("y3", d, 0), ("y3", d, 1), ("x3", d, 0), ("x3", d, 1)]
        keys += [("w", d, i) for i in range(8)]
        keys += [(k, d) for k in ("g0", "g1a", "g1b", "g2a", "g2b")]
    for k in ("t", "i"):
        keys += [(k, "in", 0), (k, "in", 1), (k, "on", 0), (k, "on", 1), (k, "far", 0), (k, "far", 1)]
        keys += [(k, "relay", 0), (k, "relay", 1)]
    return {k: i for i, k in enumerate(keys)}


def kernel(
    n, axis, keys,
    x_ref, w_ref, t_ref, lf_ref, bias_ref,
    gx_ref, gt_ref, gw_ref,
    w_all, text_low, text_in, image_low, image_in, xt, gz, from_core, to_core,
    s1a, s1b, r1a, r1b, s2a, s2b, r2a, r2b, s3a, s3b, r3a, r3b,
    send_sem, recv_sem,
):
    depth = n // 8
    opp = depth // 2
    near = [d for d in range(1, depth) if d != opp]
    rows, width = x_ref.shape
    own_rows, cols = w_ref.shape
    half = rows // 2
    ha = (cols // 128 + 1) // 2 * 128
    A, B = pl.ds(0, ha), pl.ds(ha, cols - ha)
    me = lax.axis_index(axis)
    core = lax.rem(me, 2)
    chip = me // 2
    x = lax.rem(chip, 2)
    y = lax.rem(chip // 2, 2)
    z = chip // 4

    def dev(z_, y_, x_, c_):
        return ((z_ * 2 + y_) * 2 + x_) * 2 + c_

    def up(d):
        return lax.rem(z + d, depth)

    def down(d):
        return lax.rem(z + depth - d, depth)

    xn, yn, partner = dev(z, y, 1 - x, core), dev(z, 1 - y, x, core), dev(z, y, x, 1 - core)
    sent = []
    sent_if = []

    def copy(src, dst, key, target):
        i = keys[key]
        return pltpu.make_async_remote_copy(
            src_ref=src, dst_ref=dst, send_sem=send_sem.at[i], recv_sem=recv_sem.at[i],
            device_id=(target,), device_id_type=MESH,
        )

    def send(src, dst, key, target):
        c = copy(src, dst, key, target)
        c.start()
        sent.append(c)

    def arrived(dst, key):
        copy(dst, dst, key, partner).wait_recv()

    barrier = pltpu.get_barrier_semaphore()
    first = me - core
    peers = [partner, xn, yn] + [dev(up(d), y, x, core) for d in range(1, depth)]
    peers += [lax.rem(first + n - 2 + c, n) for c in range(2)]
    peers += [lax.rem(first + 2 + c, n) for c in range(2)]
    peers += [lax.rem(me + n - 3 + 6 * core, n)]
    for peer in peers:
        pl.semaphore_signal(barrier, inc=1, device_id=(peer,), device_id_type=MESH)

    t = jnp.exp(jnp.full((1, 1), lf_ref[0], F32))
    bias = bias_ref[0]
    text = t_ref[...].astype(F32)
    text_length = jnp.sqrt(jnp.sum(text * text, axis=1, keepdims=True) + epsilon)
    text_low[...] = (text / text_length).astype(BF)
    w_all[me] = w_ref[...]

    pl.semaphore_wait(barrier, len(peers))

    send(w_ref.at[:, A], w_all.at[me, :, A], ("x1", 0), xn)
    send(w_ref.at[:, B], w_all.at[me, :, B], ("y1", 0), yn)
    for d in near:
        send(w_ref, w_all.at[me], ("z", d), dev(up(d), y, x, core))
    send(w_ref.at[:, A], w_all.at[me, :, A], ("y3", 0, 0), yn)
    send(w_ref.at[:, B], w_all.at[me, :, B], ("x3", 0, 0), xn)
    send(w_ref, w_all.at[me], ("w", 0, 0), partner)

    below, above = lax.rem(me + n - 2, n), lax.rem(me + 2, n)

    def halves(buf, slots, q, key, kind, base, cond, far=False):
        for c in range(2):
            part = pl.ds(c * half, half)
            cp = pltpu.make_async_remote_copy(
                src_ref=buf.at[part], dst_ref=slots.at[q, part],
                send_sem=send_sem.at[keys[(key, kind, c)]],
                recv_sem=recv_sem.at[keys[(key, "in", 0)] + q],
                device_id=(base + c,), device_id_type=MESH,
            )
            if far:
                arrived(slots.at[2, part], (key, "far", c))
            pl.when(cond)(cp.start)
            sent_if.append((cond, cp))

    def send_far(buf, slots, key, far):
        for c in range(2):
            part = pl.ds(c * half, half)
            send(buf.at[part], slots.at[2, part], (key, "far", c), far)

    def relay_far(slots, key, q, cond):
        halves(slots.at[2], slots, q, key, "relay", xn - core, cond, True)

    def swap_block(slots, key):
        part = pl.ds(pl.multiple_of(core * half, half), half)
        for q in range(2):
            arrived(slots.at[q, part], (key, "in", q))
            send(slots.at[q, part], slots.at[q, part], (key, "on", q), partner)

    def wait_block(slots, key, q):
        part = pl.ds(pl.multiple_of((1 - core) * half, half), half)
        arrived(slots.at[q, part], (key, "on", q))


    def onward(part, d, key_a, key_b):
        if key_a is not None and d == opp - 1:
            send(part(A), part(A), key_a, dev(up(1), y, x, core))
        if key_b is not None and d == opp + 1:
            send(part(B), part(B), key_b, dev(down(1), y, x, core))

    def step_z(d):
        s = dev(down(d), y, x, core)

        def part(cut):
            return w_all.at[s, :, cut]

        if d == opp:
            arrived(part(A), "za")
            send(part(A), part(A), ("y3", d, 0), yn)
            send(part(A), part(A), ("w", d, 0), partner)
            arrived(part(B), "zb")
            send(part(B), part(B), ("x3", d, 0), xn)
            send(part(B), part(B), ("w", d, 7), partner)
            return
        arrived(w_all.at[s], ("z", d))
        onward(part, d, "za", "zb")
        send(part(A), part(A), ("y3", d, 0), yn)
        send(part(B), part(B), ("x3", d, 0), xn)
        send(w_all.at[s], w_all.at[s], ("w", d, 0), partner)

    def step_one(d):
        def side(cut):
            return w_all.at[dev(down(d), y, 1 - x, core), :, cut]

        def front(cut):
            return w_all.at[dev(down(d), 1 - y, x, core), :, cut]

        s = side(A)
        arrived(s, ("x1", d))
        if d == 0:
            for e in near:
                send(s, s, ("x1", e), dev(up(e), y, x, core))
        onward(side, d, ("x1", opp), None)
        send(s, s, ("y3", d, 1), yn)
        send(s, s, ("w", d, 1), partner)
        s = front(B)
        arrived(s, ("y1", d))
        if d == 0:
            for e in near:
                send(s, s, ("y1", e), dev(up(e), y, x, core))
        onward(front, d, None, ("y1", opp))
        send(s, s, ("x3", d, 1), xn)
        send(s, s, ("w", d, 2), partner)

    def step_two(d):
        for i, x_ in enumerate((x, 1 - x)):
            s = w_all.at[dev(down(d), 1 - y, x_, core), :, A]
            arrived(s, ("y3", d, i))
            send(s, s, ("w", d, 3 + i), partner)
        for i, y_ in enumerate((y, 1 - y)):
            s = w_all.at[dev(down(d), y_, 1 - x, core), :, B]
            arrived(s, ("x3", d, i))
            send(s, s, ("w", d, 5 + i), partner)

    send_far(text_low, text_in, "t", lax.rem(me + n - 3 + 2 * core, n))
    step_one(0)
    for d in near:
        step_z(d)
    passed_on = jnp.logical_and(x == 0, core == 0)
    halves(text_low, text_in, core, "t", "in", below - core, jnp.logical_not(passed_on))
    for d in near:
        step_one(d)
    relay_far(text_in, "t", 0, jnp.logical_and(x == 0, core == 1))
    step_z(opp)
    step_one(opp)
    for d in [0] + near + [opp]:
        step_two(d)

    xt[...] = x_ref[...].T

    other = 1 - core
    for d in range(depth):
        zs = down(d)
        if d == opp:
            arrived(w_all.at[dev(zs, y, x, other), :, A], ("w", d, 0))
            arrived(w_all.at[dev(zs, y, x, other), :, B], ("w", d, 7))
        else:
            arrived(w_all.at[dev(zs, y, x, other)], ("w", d, 0))
        arrived(w_all.at[dev(zs, y, 1 - x, other), :, A], ("w", d, 1))
        arrived(w_all.at[dev(zs, 1 - y, x, other), :, B], ("w", d, 2))
        for i, x_ in enumerate((x, 1 - x)):
            arrived(w_all.at[dev(zs, 1 - y, x_, other), :, A], ("w", d, 3 + i))
        for i, y_ in enumerate((y, 1 - y)):
            arrived(w_all.at[dev(zs, y_, 1 - x, other), :, B], ("w", d, 5 + i))

    weight = w_all[...].reshape(n * own_rows, cols)
    embedded = jnp.dot(x_ref[...], weight, preferred_element_type=F32)
    image_length = jnp.sqrt(jnp.sum(embedded * embedded, axis=1, keepdims=True) + epsilon)
    image_unit = embedded / image_length
    image_low[...] = image_unit.astype(BF)
    mine = image_low[...]
    own_text = text_low[...]

    grad = pair_grad(mine, own_text, t, bias, True)
    image_grad = jnp.dot(grad, own_text, preferred_element_type=F32)
    send_far(image_low, image_in, "i", lax.rem(me + 1 + 2 * core, n))
    passed_on = jnp.logical_and(x == 1, core == 1)
    halves(image_low, image_in, core, "i", "in", above - core, jnp.logical_not(passed_on))

    swap_block(text_in, "t")
    for q in (2, 0, 1):
        if q < 2:
            wait_block(text_in, "t", q)
        block = text_in[q]
        image_grad += jnp.dot(
            pair_grad(mine, block, t, bias, False), block, preferred_element_type=F32
        )
    along = jnp.sum(image_unit * image_grad, axis=1, keepdims=True)
    embed_grad = ((image_grad - image_unit * along) / image_length).astype(BF)

    order = [opp] + near + [0]
    group = 8 * own_rows
    for d in order:
        lhs = xt[pl.ds(pl.multiple_of(up(d) * group, group), group), :]
        part = jnp.dot(lhs, embed_grad, preferred_element_type=F32)
        gz[d] = part.reshape(4, 2, own_rows, cols)
        for c in range(4):
            to_core[d, c] = gz[d, c, other].astype(BF)
        send(to_core.at[d], from_core.at[d], ("g0", d), partner)

    def base(d, c, cut):
        return gz[d, c, core, :, cut] + from_core[d, c, :, cut].astype(F32)

    relay_far(image_in, "i", 1, jnp.logical_and(x == 1, core == 0))
    gx_ref[...] = dot_nt(embed_grad, weight).astype(BF)

    for d in order:
        arrived(from_core.at[d], ("g0", d))
        for i in range(2):
            s1a[d, i] = base(d, (1 - y) * 2 + i, A).astype(BF)
            s1b[d, i] = base(d, i * 2 + 1 - x, B).astype(BF)
        send(s1a.at[d], r1a.at[d], ("g1a", d), yn)
        send(s1b.at[d], r1b.at[d], ("g1b", d), xn)

    text_grad = jnp.dot(
        pair_grad(own_text, mine, t, bias, True), mine, preferred_element_type=F32
    )

    def stage_two(d):
        arrived(r1a.at[d], ("g1a", d))
        arrived(r1b.at[d], ("g1b", d))
        if d == opp - 1:
            arrived(r2a.at[opp], ("g2a", opp))
        if d == opp + 1:
            arrived(r2b.at[opp], ("g2b", opp))
        for i in range(2):
            left = base(d, y * 2 + i, A) + r1a[d, i].astype(F32)
            right = base(d, i * 2 + x, B) + r1b[d, i].astype(F32)
            if d == opp - 1:
                left += r2a[opp, i].astype(F32)
            if d == opp + 1:
                right += r2b[opp, i].astype(F32)
            s2a[d, i] = left.astype(BF)
            s2b[d, i] = right.astype(BF)
        ta, tb = (up(1), down(1)) if d == opp else (up(d), up(d))
        send(s2a.at[d], r2a.at[d], ("g2a", d), dev(ta, y, x, core))
        send(s2b.at[d], r2b.at[d], ("g2b", d), dev(tb, y, x, core))

    def gathered(i, j):
        left = base(0, y * 2 + i, A) + r1a[0, i].astype(F32)
        right = base(0, j * 2 + x, B) + r1b[0, j].astype(F32)
        for d in near:
            left += r2a[d, i].astype(F32)
            right += r2b[d, j].astype(F32)
        return left, right

    swap_block(image_in, "i")
    for d in [opp] + near:
        stage_two(d)

    for q in (2, 0, 1):
        if q < 2:
            wait_block(image_in, "i", q)
        block = image_in[q]
        text_grad += jnp.dot(
            pair_grad(own_text, block, t, bias, False), block, preferred_element_type=F32
        )
    arrived(r1a.at[0], ("g1a", 0))
    arrived(r1b.at[0], ("g1b", 0))
    for d in near:
        arrived(r2a.at[d], ("g2a", d))
        arrived(r2b.at[d], ("g2b", d))
    left, right = gathered(1 - x, 1 - y)
    s3a[...] = left.astype(BF)
    s3b[...] = right.astype(BF)
    send(s3a, r3a, "g3a", xn)
    send(s3b, r3b, "g3b", yn)
    left, right = gathered(x, y)
    gw_ref[:, A] = left
    gw_ref[:, B] = right
    text_unit = t_ref[...].astype(F32) / text_length
    along = jnp.sum(text_unit * text_grad, axis=1, keepdims=True)
    gt_ref[...] = ((text_grad - text_unit * along) / text_length).astype(BF)

    arrived(r3a, "g3a")
    arrived(r3b, "g3b")
    gw_ref[:, A] += r3a[...].astype(F32)
    gw_ref[:, B] += r3b[...].astype(F32)
    for c in sent:
        c.wait_send()
    for cond, c in sent_if:
        pl.when(cond)(c.wait_send)


def fused(n, axis, image_features, head_weight, text_embeds, factor, bias):
    depth = n // 8
    rows, width = image_features.shape
    own_rows, cols = head_weight.shape
    keys = sem_keys(depth)
    ha = (cols // 128 + 1) // 2 * 128
    hb = cols - ha
    vmem = pl.BlockSpec(memory_space=pltpu.VMEM)
    smem = pl.BlockSpec(memory_space=pltpu.SMEM)
    scratch = [
        ((n, own_rows, cols), BF),
        ((rows, cols), BF),
        ((3, rows, cols), BF),
        ((rows, cols), BF),
        ((3, rows, cols), BF),
        ((width, rows), BF),
        ((depth, 4, 2, own_rows, cols), F32),
        ((depth, 4, own_rows, cols), BF),
        ((depth, 4, own_rows, cols), BF),
        ((depth, 2, own_rows, ha), BF),
        ((depth, 2, own_rows, hb), BF),
        ((depth, 2, own_rows, ha), BF),
        ((depth, 2, own_rows, hb), BF),
        ((depth, 2, own_rows, ha), BF),
        ((depth, 2, own_rows, hb), BF),
        ((depth, 2, own_rows, ha), BF),
        ((depth, 2, own_rows, hb), BF),
        ((own_rows, ha), BF),
        ((own_rows, hb), BF),
        ((own_rows, ha), BF),
        ((own_rows, hb), BF),
    ]
    return pl.pallas_call(
        functools.partial(kernel, n, axis, keys),
        out_shape=(
            jax.ShapeDtypeStruct((rows, width), BF),
            jax.ShapeDtypeStruct((rows, cols), BF),
            jax.ShapeDtypeStruct((own_rows, cols), F32),
        ),
        in_specs=[vmem, vmem, vmem, smem, smem],
        out_specs=(vmem, vmem, vmem),
        scratch_shapes=[pltpu.VMEM(s, d) for s, d in scratch]
        + [pltpu.SemaphoreType.DMA((len(keys),))] * 2,
        compiler_params=pltpu.CompilerParams(
            collective_id=0, has_side_effects=True, vmem_limit_bytes=60 * 2**20
        ),
    )(image_features, head_weight, text_embeds, factor, bias)


def passed_along(block, axis, distance):
    devices = range(lax.axis_size(axis))
    route = [((i - distance) % len(devices), i) for i in devices]
    return lax.ppermute(block, axis, route)


def normalize(rows):
    squares = jnp.sum(rows * rows, axis=1, keepdims=True)
    length = jnp.sqrt(squares + epsilon)
    return (rows / length, length)


def similarity_derivative(
    picture_sample_group,
    caption_sample_group,
    similarity_multiplier,
    neighbour_distance,
    outer_dimension_size,
):
    similarity_matrix = (
        similarity_multiplier
        * lax.dot_general(
            picture_sample_group,
            caption_sample_group,
            (((1,), (1,)), ((), ())),
            preferred_element_type=jnp.float32,
        )
        + neighbour_distance
    )
    if outer_dimension_size:
        matched = lax.broadcasted_iota(
            jnp.int32, similarity_matrix.shape, 0
        ) == lax.broadcasted_iota(jnp.int32, similarity_matrix.shape, 1)
        match_polarity = jnp.where(matched, 1.0, -1.0).astype(jnp.float32)
    else:
        match_polarity = -jnp.ones(similarity_matrix.shape, jnp.float32)
    return (
        -similarity_multiplier
        * match_polarity
        * jax.nn.sigmoid(-match_polarity * similarity_matrix)
    ).astype(jnp.bfloat16)


def project_back(grad, unit_rows, length):
    return (grad - unit_rows * jnp.sum(unit_rows * grad, axis=1, keepdims=True)) / length


def by_collectives(image_features, head_weight, text_embeds, natural_exponent_factor, logit_bias):
    full_weight = lax.all_gather(head_weight, "blk", axis=0, tiled=True)
    embedded = jnp.dot(image_features, full_weight, preferred_element_type=jnp.float32)
    image_unit, image_length = normalize(embedded)
    picture_embedding_mapped = image_unit.astype(jnp.bfloat16)
    text_unit, text_length = normalize(text_embeds.astype(jnp.float32))
    text_low = text_unit.astype(jnp.bfloat16)
    similarity_multiplier = jnp.exp(natural_exponent_factor[0])
    neighbour_distance = logit_bias[0]
    image_grad = jnp.zeros(image_unit.shape, jnp.float32)
    current_neighbour_tile = text_low
    for partition_portion in range(S):
        mapping_matrix = similarity_derivative(
            picture_embedding_mapped,
            current_neighbour_tile,
            similarity_multiplier,
            neighbour_distance,
            partition_portion == 0,
        )
        image_grad = image_grad + jnp.dot(
            mapping_matrix, current_neighbour_tile, preferred_element_type=jnp.float32
        )
        if partition_portion + 1 < S:
            current_neighbour_tile = passed_along(current_neighbour_tile, "blk", -1)
    text_grad = jnp.zeros(text_unit.shape, jnp.float32)
    passing = picture_embedding_mapped
    for partition_portion in range(S):
        mapping_matrix = similarity_derivative(
            passing, text_low, similarity_multiplier, neighbour_distance, partition_portion == 0
        )
        text_grad = text_grad + lax.dot_general(
            mapping_matrix, passing, (((0,), (0,)), ((), ())), preferred_element_type=jnp.float32
        )
        if partition_portion + 1 < S:
            passing = passed_along(passing, "blk", 1)
    embed_grad = project_back(image_grad, image_unit, image_length).astype(jnp.bfloat16)
    grad_text = project_back(text_grad, text_unit, text_length).astype(jnp.bfloat16)
    grad_features = lax.dot_general(
        embed_grad, full_weight, (((1,), (1,)), ((), ())), preferred_element_type=jnp.float32
    ).astype(jnp.bfloat16)
    grad_weight = lax.psum_scatter(
        lax.dot_general(
            image_features, embed_grad, (((0,), (0,)), ((), ())), preferred_element_type=jnp.float32
        ),
        "blk",
        scatter_dimension=0,
        tiled=True,
    )
    return (grad_features, grad_text, grad_weight)


def on_device(image_features, head_weight, text_embeds, natural_exponent_factor, logit_bias):
    n = lax.axis_size("blk")
    whole_tiles = head_weight.shape[0] % 16 == 0 and n % 16 == 0 and n > 16
    run = functools.partial(fused, n, "blk") if whole_tiles else by_collectives
    return run(image_features, head_weight, text_embeds, natural_exponent_factor, logit_bias)


def solution(mesh):
    return jax.shard_map(
        on_device,
        mesh=mesh,
        in_specs=(P("blk", None), P("blk", None), P("blk", None), P(), P()),
        out_specs=(P("blk", None), P("blk", None), P("blk", None)),
        check_vma=False,
    )
```
